32 devices in a mesh: dp: 4 (over z), tp: 8 (over y, x, core).
Axes of the slice: x: 2, y: 2, z: 4, core: 2. Of those that a mesh axis runs over, the one named last changes fastest.
Arguments:
- token_ids: int32 [32768], P('dp'), parts along dimension 0
- positions: int32 [32768], P('dp'), parts along dimension 0
- embed_table: bfloat16 [257216, 2048], P('tp')
- norm_scale: float32 [2048], replicated
- w_query: bfloat16 [2048, 2048], P(None, 'tp')
- w_key: bfloat16 [2048, 256], replicated
- w_value: bfloat16 [2048, 256], replicated
Outputs:
- output 1: bfloat16 [32768, 2048], P(('dp', 'tp')), parts along dimension 0
- output 2: bfloat16 [32768, 8, 256], P('dp', 'tp'), parts along dimension 0
- output 3: bfloat16 [32768, 8, 256], P('dp', 'tp'), parts along dimension 0
- output 4: bfloat16 [32768, 8, 256], P('dp', 'tp'), parts along dimension 0
There are 4 independent parts. The reference program is written for one: setup_inputs(seed, part) draws one part's arguments, and reference() takes and returns one part's arrays. A program takes and returns all parts, laid end to end along the dimension named above; an argument that names none is the same for every part.
All inputs are finite; a program needn't handle non-finite values.
Results may differ from the reference program's by a relative error of at most 0.0120334.
Values are sent between devices in bfloat16 or wider.
A program may use at most 1 GiB of HBM per device.

```python
import math
import numpy as np
import jax
import jax.numpy as jnp
from jax import lax

D = 2048
HEADS = 8
KV_HEADS = 1
VOCAB = 257216
HEAD_DIM = 256
TOKENS = 8192
KV_SLOTS = 8
START_ODDS = 256
LEVELS = 16

ID_CAPS = np.minimum(VOCAB, 16 * 2 ** np.arange(LEVELS))


def draw_ids(key):
    level_key, id_key = jax.random.split(key)
    levels_drawn = jax.random.randint(level_key, (TOKENS,), 0, LEVELS)
    upper_ids = jnp.asarray(ID_CAPS, dtype=jnp.int32)[levels_drawn]
    token_ids = jax.random.randint(id_key, (TOKENS,), 0, upper_ids, dtype=jnp.int32)
    return token_ids.at[0].set(VOCAB - 1).at[1].set(0)


def draw_positions(key):
    step_ids = jnp.arange(TOKENS, dtype=jnp.int32)
    is_start = jax.random.randint(key, (TOKENS,), 0, START_ODDS, dtype=jnp.int32) == 0
    is_start = is_start.at[0].set(True)
    start_ids = lax.cummax(jnp.where(is_start, step_ids, 0), axis=0)
    return step_ids - start_ids


def setup_inputs(seed: int = 0, part: int = 0) -> dict:
    root_key = jax.random.key(seed)
    part_key = jax.random.fold_in(root_key, part)
    id_key, pos_key = jax.random.split(part_key)
    shared = jax.random.split(root_key, 6)
    row_scale = jax.random.uniform(shared[0], (VOCAB, 1), jnp.float32, 0.25, 2.0)
    embed_table = (jax.random.normal(shared[1], (VOCAB, D), jnp.float32) * (row_scale * D ** -0.5)).astype(jnp.bfloat16)
    norm_scale = 0.5 * jax.random.normal(shared[2], (D,), jnp.float32)
    w_query = (jax.random.normal(shared[3], (D, HEADS * HEAD_DIM), jnp.float32) * D ** -0.5).astype(jnp.bfloat16)
    w_key = (jax.random.normal(shared[4], (D, KV_HEADS * HEAD_DIM), jnp.float32) * D ** -0.5).astype(jnp.bfloat16)
    w_value = (jax.random.normal(shared[5], (D, KV_HEADS * HEAD_DIM), jnp.float32) * D ** -0.5).astype(jnp.bfloat16)
    return {"token_ids": draw_ids(id_key), "positions": draw_positions(pos_key), "embed_table": embed_table, "norm_scale": norm_scale, "w_query": w_query, "w_key": w_key, "w_value": w_value}


def rotate(head_vals, cosines, sines):
    half_dim = HEAD_DIM // 2
    front_half = head_vals[..., :half_dim]
    back_half = head_vals[..., half_dim:]
    return jnp.concatenate([front_half * cosines - back_half * sines, back_half * cosines + front_half * sines], axis=-1)


def reference(token_ids, positions, embed_table, norm_scale, w_query, w_key, w_value):
    normalizer = jnp.asarray(math.sqrt(D), dtype=jnp.bfloat16)
    residual = jnp.take(embed_table, token_ids, axis=0) * normalizer
    widened = residual.astype(jnp.float32)
    inv_rms = lax.rsqrt(jnp.mean(widened * widened, axis=-1, keepdims=True) + 1e-6)
    normed = (widened * inv_rms * (1.0 + norm_scale)).astype(jnp.bfloat16)
    inv_freq = 10000.0 ** (-jnp.arange(0, HEAD_DIM, 2, dtype=jnp.float32) / HEAD_DIM)
    angles = positions.astype(jnp.float32)[:, None] * inv_freq[None, :]
    cosines = jnp.cos(angles)[:, None, :]
    sines = jnp.sin(angles)[:, None, :]
    q_lin = jnp.dot(normed, w_query, preferred_element_type=jnp.float32).astype(jnp.bfloat16)
    k_lin = jnp.dot(normed, w_key, preferred_element_type=jnp.float32).astype(jnp.bfloat16)
    v_lin = jnp.dot(normed, w_value, preferred_element_type=jnp.float32).astype(jnp.bfloat16)
    queries = (rotate(q_lin.reshape(TOKENS, HEADS, HEAD_DIM).astype(jnp.float32), cosines, sines) * HEAD_DIM ** -0.5).astype(jnp.bfloat16)
    keys_rot = rotate(k_lin.reshape(TOKENS, KV_HEADS, HEAD_DIM).astype(jnp.float32), cosines, sines).astype(jnp.bfloat16)
    repeats = KV_SLOTS // KV_HEADS
    key_heads = jnp.repeat(keys_rot, repeats, axis=1)
    value_heads = jnp.repeat(v_lin.reshape(TOKENS, KV_HEADS, HEAD_DIM), repeats, axis=1)
    return (residual, queries, key_heads, value_heads)
```

```python
import functools
import math

import jax
import numpy as np
import jax.numpy as jnp
from jax import lax
from jax.experimental import pallas as pl
from jax.experimental.pallas import tpu as pltpu
from jax.sharding import PartitionSpec as P

HEAD_DIM = 256
EPSILON = 1e-6
ROPE_BASE = 10000.0
MESH = pl.DeviceIdType.MESH
BF16, F32, I32 = jnp.bfloat16, jnp.float32, jnp.int32

HOT = 1024
LIST_CAP = (2816, 640, 352, 352, 192, 192, 192, 192)
CHUNK = (64, 64, 32, 32, 32, 32, 32, 32)
SEG_ROWS = tuple(c + (HOT if d == 0 else 0) for d, c in enumerate(LIST_CAP))
SEG_BASE = tuple(sum(SEG_ROWS[:d]) for d in range(8))
TOTAL = sum(SEG_ROWS)
ROWS = -(-TOTAL // 256) * 256
SEG_CHUNKS = tuple(r // c for r, c in zip(SEG_ROWS, CHUNK))
CHUNK_ID = tuple(sum(SEG_CHUNKS[:d]) for d in range(8))
ALL_CHUNKS = sum(SEG_CHUNKS)
SPLIT = 35
LIST_LEN = 3072
RING = ((0, 1, 3, 2), (0, 2, 3, 1))


def rope_tables(positions):
    inv_freq = ROPE_BASE ** (-jnp.arange(0, HEAD_DIM, 2, dtype=F32) / HEAD_DIM)
    angles = positions.astype(F32)[:, None] * inv_freq[None, :]
    return jnp.cos(angles), jnp.sin(angles)


def rotate(head_vals, cosines, sines):
    half_dim = head_vals.shape[-1] // 2
    front_half = head_vals[..., :half_dim]
    back_half = head_vals[..., half_dim:]
    return jnp.concatenate([front_half * cosines - back_half * sines, back_half * cosines + front_half * sines], axis=-1)


def rms_norm(resid_rows, norm_scale):
    widened = resid_rows.astype(F32)
    inv_rms = lax.rsqrt(jnp.mean(widened * widened, axis=-1, keepdims=True) + EPSILON)
    return (widened * inv_rms * (1.0 + norm_scale)).astype(BF16)


def dense_step(token_ids, positions, table_rows, norm_scale, w_query, w_key, w_value):
    vocab_rows, model_width = table_rows.shape
    normalizer = jnp.asarray(math.sqrt(model_width), dtype=BF16)
    local_ids = token_ids - lax.axis_index("tp") * vocab_rows
    inside = (local_ids >= 0) & (local_ids < vocab_rows)
    picked = jnp.take(table_rows, local_ids, axis=0, mode="clip") * normalizer
    partial = jnp.where(inside[:, None], picked, jnp.zeros((), BF16))
    residual = lax.psum_scatter(partial, "tp", scatter_dimension=0, tiled=True)
    normed = lax.all_gather(rms_norm(residual, norm_scale), "tp", axis=0, tiled=True)
    cosines, sines = rope_tables(positions)

    def project(weight, factor):
        linear = jnp.dot(normed, weight, preferred_element_type=F32).astype(BF16).astype(F32)
        return (rotate(linear, cosines, sines) * factor).astype(BF16)

    value_heads = jnp.dot(normed, w_value, preferred_element_type=F32).astype(BF16)
    return residual, project(w_query, HEAD_DIM ** -0.5), project(w_key, 1.0), value_heads


def plan(token_ids, vocab_rows, me):
    tokens = token_ids.shape[0]
    lanes = 128
    ids = token_ids.reshape(tokens // lanes, lanes)
    owner = ids // vocab_rows
    hot = ids < HOT
    mine = jnp.where(hot, 8, owner)
    onehot = mine[None] == jnp.arange(8, dtype=I32)[:, None, None]
    marks = onehot.astype(BF16)
    upper = (jnp.arange(lanes)[:, None] < jnp.arange(lanes)[None, :]).astype(BF16)
    within = jnp.einsum("orl,lm->orm", marks, upper, preferred_element_type=F32)
    per_row = jnp.sum(onehot.astype(F32), axis=-1)
    rows = tokens // lanes
    lower = (jnp.arange(rows)[None, :] < jnp.arange(rows)[:, None]).astype(F32)
    before = jnp.sum(lower[None] * per_row[:, None, :], axis=-1)
    counts = jnp.sum(per_row, axis=-1).astype(I32)
    place = (within + before[:, :, None]).astype(I32)
    bases = jnp.asarray([SEG_BASE[d] + (HOT if d == 0 else 0) for d in range(8)], I32)
    index = jnp.sum(jnp.where(onehot, place + bases[:, None, None], 0), axis=0)
    index = jnp.where(hot, ids, index).reshape(tokens)
    caps = jnp.asarray(LIST_CAP, I32)
    fits = jnp.all(counts <= caps)
    index = jnp.minimum(index, ROWS - 1)

    own = mine == me
    own_place = jnp.sum(jnp.where(onehot, place, 0), axis=0).reshape(tokens)
    own = own.reshape(tokens)
    local = jnp.where(own, token_ids - me * vocab_rows, 0)
    tall = LIST_LEN // 64
    high = (own[:, None] & (own_place[:, None] // 64 == jnp.arange(tall)[None, :])).astype(BF16)
    low = (own_place[:, None] % 64 == jnp.arange(64)[None, :]).astype(F32)
    values = jnp.concatenate([low * (local // 256).astype(F32)[:, None], low * (local % 256).astype(F32)[:, None]], axis=1)
    table = lax.dot_general(high, values.astype(BF16), (((0,), (0,)), ((), ())), preferred_element_type=F32)
    own_list = (table[:, :64] * 256 + table[:, 64:]).astype(I32).reshape(LIST_LEN)
    count = jnp.minimum(jnp.sum(own.astype(I32)), caps[me])
    return index, own_list, count, fits


STEP = 128


def gather_kernel(scale, params, rows_list, lanes_list, source, out, groups, picked, in_sems, out_sems):
    hot_steps, steps, base = params[0], params[1], params[2]
    end = hot_steps + steps

    def issue(step, slot):
        @pl.when(step < hot_steps)
        def _():
            pltpu.make_async_copy(source.at[pl.ds(pl.multiple_of(step * STEP, STEP), STEP)], groups.at[slot, pl.ds(0, STEP)], in_sems.at[slot]).start()

        @pl.when(step >= hot_steps)
        def _():
            def one(t, _):
                group = lax.div(rows_list[(step - hot_steps) * STEP + t], 8)
                pltpu.make_async_copy(source.at[pl.ds(pl.multiple_of(group * 8, 8), 8)], groups.at[slot, pl.ds(pl.multiple_of(t * 8, 8), 8)], in_sems.at[slot]).start()
                return 0

            lax.fori_loop(0, STEP, one, 0, unroll=8)

    def drain(slot):
        pltpu.make_async_copy(picked.at[slot], out.at[pl.ds(0, STEP)], out_sems.at[slot]).wait()

    @pl.when(end > 0)
    def _():
        issue(0, 0)

    def body(step, _):
        slot = lax.rem(step, 2)

        @pl.when(step + 1 < end)
        def _():
            issue(step + 1, 1 - slot)

        @pl.when(step >= 2)
        def _():
            drain(slot)

        @pl.when(step < hot_steps)
        def _():
            pltpu.make_async_copy(source.at[pl.ds(0, STEP)], groups.at[slot, pl.ds(0, STEP)], in_sems.at[slot]).wait()
            picked[slot] = groups[slot, :STEP, :]

        @pl.when(step >= hot_steps)
        def _():
            pltpu.make_async_copy(source.at[pl.ds(0, STEP * 8)], groups.at[slot], in_sems.at[slot]).wait()
            within = lax.rem(lanes_list[pl.ds(step - hot_steps, 1), :], 8)
            target = lax.broadcasted_iota(I32, (1, STEP), 1) * 8 + within
            target = jnp.broadcast_to(target, (STEP, STEP)).T
            lane = lax.broadcasted_iota(I32, (STEP, STEP), 1)
            select = jnp.concatenate([(lane + STEP * j == target).astype(F32).astype(BF16) for j in range(8)], axis=1)
            for c in range(0, 2048, 256):
                rows = jnp.dot(select, groups[slot, :, c:c + 256], preferred_element_type=F32)
                picked[slot, :, c:c + 256] = (rows if scale is None else rows * scale).astype(BF16)

        pltpu.make_async_copy(picked.at[slot], out.at[pl.ds(pl.multiple_of(base + step * STEP, 8), STEP)], out_sems.at[slot]).start()
        return 0

    lax.fori_loop(0, end, body, 0)

    @pl.when(end >= 2)
    def _():
        drain(lax.rem(end, 2))

    @pl.when(end >= 1)
    def _():
        drain(lax.rem(end + 1, 2))


def gather_rows(params, rows_list, source, out_rows, scale, name):
    return pl.pallas_call(
        functools.partial(gather_kernel, scale),
        out_shape=jax.ShapeDtypeStruct((out_rows, source.shape[1]), BF16),
        in_specs=[
            pl.BlockSpec(memory_space=pltpu.SMEM),
            pl.BlockSpec(memory_space=pltpu.SMEM),
            pl.BlockSpec(memory_space=pltpu.VMEM),
            pl.BlockSpec(memory_space=pl.ANY),
        ],
        out_specs=pl.BlockSpec(memory_space=pl.ANY),
        scratch_shapes=[
            pltpu.VMEM((2, STEP * 8, 2048), BF16),
            pltpu.VMEM((2, STEP, 2048), BF16),
            pltpu.SemaphoreType.DMA((2,)),
            pltpu.SemaphoreType.DMA((2,)),
        ],
        name=name,
    )(params, rows_list, rows_list.reshape(-1, STEP), source)


def ring_device(core, place):
    return 2 * RING[core][place % 4] + core


def ring_parts(core, place):
    if place % 4:
        device = ring_device(core, place)
        return [(device, 0, SEG_CHUNKS[device])]
    if core == 0:
        return [(0, 0, SPLIT)]
    return [(1, 0, SEG_CHUNKS[1]), (0, SPLIT, SEG_CHUNKS[0] - SPLIT)]


def broadcast_kernel(_, rows, ring_sems, pair_sems, recv_sems):
    me = lax.axis_index("tp")
    core, chip = me % 2, me // 2
    x, y = chip % 2, chip // 2
    along_x = 2 * (2 * y + 1 - x) + core
    along_y = 2 * (2 * (1 - y) + x) + core
    other = 2 * chip + 1 - core
    barrier = pltpu.get_barrier_semaphore()
    for peer in (along_x, along_y, other):
        pl.semaphore_signal(barrier, inc=1, device_id={"tp": peer}, device_id_type=MESH)
    pl.semaphore_wait(barrier, 3)

    def chunk(device, i):
        size = CHUNK[device]
        return rows.at[pl.ds(pl.multiple_of(SEG_BASE[device] + i * size, 8), size)], CHUNK_ID[device] + i

    def copy(device, i, sems, target):
        ref, number = chunk(device, i)
        return pltpu.make_async_remote_copy(
            src_ref=ref, dst_ref=ref, send_sem=sems.at[number], recv_sem=recv_sems.at[number],
            device_id={"tp": target}, device_id_type=MESH)

    def each(parts, fn):
        for device, first, number in parts:
            def body(i, _, device=device):
                fn(device, i)
                return 0

            lax.fori_loop(first, first + number, body, 0)

    def role(core, place):
        here = ring_device(core, place)
        after, pair = ring_device(core, place + 1), here ^ 1

        def to_ring(device, i):
            copy(device, i, ring_sems, after).start()

        def to_pair(device, i):
            copy(device, i, pair_sems, pair).start()

        def arrived(device, i):
            copy(device, i, ring_sems, after).wait_recv()

        def to_both(device, i):
            to_ring(device, i)
            to_pair(device, i)

        def arrive_to_both(device, i):
            arrived(device, i)
            to_both(device, i)

        def arrive_to_ring(device, i):
            arrived(device, i)
            to_ring(device, i)

        def arrive_to_pair(device, i):
            arrived(device, i)
            to_pair(device, i)

        own = [(here, 0, SEG_CHUNKS[here])]
        head = ring_parts(core, place)
        late = []
        if here == 0:
            late = ring_parts(1, 0)[1:]
            both = min(late[0][2], SPLIT)

            def interleave(i, _):
                to_pair(0, SPLIT + i)
                to_both(0, i)
                return 0

            lax.fori_loop(0, both, interleave, 0)
            each([(0, both, SPLIT - both)], to_both)
            each([(0, SPLIT + both, late[0][2] - both)], to_pair)
            sent_ring, sent_pair = list(head), list(own)
        elif here == 1:
            each(own, to_both)
            each(head[1:], arrive_to_ring)
            sent_ring, sent_pair = list(head), list(own)
        else:
            each(own, to_both)
            sent_ring, sent_pair = list(own), list(own)
        for back in (1, 2):
            parts = ring_parts(core, place - back)
            each(parts, arrive_to_both)
            sent_ring += parts
            sent_pair += parts
        parts = ring_parts(core, place - 3)
        each(parts, arrive_to_pair)
        sent_pair += parts
        pair_place = RING[1 - core].index(here // 2)
        if here == 1:
            from_pair = [(0, 0, SPLIT)]
        elif here == 0:
            from_pair = [(1, 0, SEG_CHUNKS[1])]
        else:
            from_pair = ring_parts(1 - core, pair_place)
        for back in (1, 2, 3):
            from_pair = from_pair + ring_parts(1 - core, pair_place - back)
        each(from_pair, arrived)
        each(sent_ring, lambda device, i: copy(device, i, ring_sems, after).wait_send())
        each(sent_pair, lambda device, i: copy(device, i, pair_sems, pair).wait_send())

    for core_here in range(2):
        for place_here in range(4):
            pl.when(me == ring_device(core_here, place_here))(functools.partial(role, core_here, place_here))


def broadcast_rows(rows):
    return pl.pallas_call(
        broadcast_kernel,
        out_shape=jax.ShapeDtypeStruct(rows.shape, rows.dtype),
        in_specs=[pl.BlockSpec(memory_space=pl.ANY)],
        out_specs=pl.BlockSpec(memory_space=pl.ANY),
        scratch_shapes=[
            pltpu.SemaphoreType.DMA((ALL_CHUNKS,)),
            pltpu.SemaphoreType.DMA((ALL_CHUNKS,)),
            pltpu.SemaphoreType.DMA((ALL_CHUNKS,)),
        ],
        input_output_aliases={0: 0},
        compiler_params=pltpu.CompilerParams(collective_id=0, has_side_effects=True),
        name="broadcast_rows",
    )(rows)


ROW_BLOCK = 256
TOKEN_BLOCK = 256
PITCH = ROWS + 8
OUT_PITCH = TOKEN_BLOCK + 8
ROW_STEPS = ROWS // ROW_BLOCK


def project_kernel(scale, index, rows, norm_scale, w_query, w_key, w_value, cosines, sines, q_out, k_out, v_out, linear, turned):
    step = pl.program_id(0)

    @pl.when(step < ROW_STEPS)
    def _():
        resid = (rows[...].astype(F32) * scale).astype(BF16).astype(F32)
        inv_rms = lax.rsqrt(jnp.mean(resid * resid, axis=-1, keepdims=True) + EPSILON)
        normed = (resid * inv_rms * (1.0 + norm_scale[...])).astype(BF16)
        for which, weight in enumerate((w_query, w_key, w_value)):
            product = jnp.dot(normed, weight[...], preferred_element_type=F32).astype(BF16).astype(F32)
            for half in range(2):
                at = pl.multiple_of((2 * which + half) * PITCH + step * ROW_BLOCK, 8)
                linear[pl.ds(at, ROW_BLOCK), :] = product[:, 128 * half:128 * half + 128]

    @pl.when(step >= ROW_STEPS)
    def _():
        first = (step - ROW_STEPS) * TOKEN_BLOCK

        def some(i, _):
            for u in range(16):
                t = i * 16 + u
                row = index[first + t]
                turned[pl.ds(t, 8, stride=OUT_PITCH), :] = linear[pl.ds(row, 8, stride=PITCH), :]
            return 0

        lax.fori_loop(0, TOKEN_BLOCK // 16, some, 0)
        part = [turned[OUT_PITCH * j:OUT_PITCH * j + TOKEN_BLOCK, :] for j in range(6)]
        cos, sin = cosines[...], sines[...]
        factor = HEAD_DIM ** -0.5
        q_out[:, :128] = ((part[0] * cos - part[1] * sin) * factor).astype(BF16)
        q_out[:, 128:] = ((part[1] * cos + part[0] * sin) * factor).astype(BF16)
        k_out[:, :128] = (part[2] * cos - part[3] * sin).astype(BF16)
        k_out[:, 128:] = (part[3] * cos + part[2] * sin).astype(BF16)
        v_out[:, :128] = part[4].astype(BF16)
        v_out[:, 128:] = part[5].astype(BF16)


def project(index, rows, norm_scale, w_query, w_key, w_value, cosines, sines, scale):
    tokens = index.shape[0]
    token_steps = tokens // TOKEN_BLOCK
    whole = lambda i, idx: (0, 0)
    by_token = lambda i, idx: (jnp.maximum(i - ROW_STEPS, 0), 0)
    out = jax.ShapeDtypeStruct((tokens, HEAD_DIM), BF16)
    weight = pl.BlockSpec((2048, HEAD_DIM), whole)
    return pl.pallas_call(
        functools.partial(project_kernel, scale),
        out_shape=(out, out, out),
        grid_spec=pltpu.PrefetchScalarGridSpec(
            num_scalar_prefetch=1,
            grid=(ROW_STEPS + token_steps,),
            in_specs=[
                pl.BlockSpec((ROW_BLOCK, 2048), lambda i, idx: (jnp.minimum(i, ROW_STEPS - 1), 0)),
                pl.BlockSpec((1, 2048), whole), weight, weight, weight,
                pl.BlockSpec((TOKEN_BLOCK, 128), by_token),
                pl.BlockSpec((TOKEN_BLOCK, 128), by_token),
            ],
            out_specs=[pl.BlockSpec((TOKEN_BLOCK, HEAD_DIM), by_token)] * 3,
            scratch_shapes=[pltpu.VMEM((8 * PITCH, 128), F32), pltpu.VMEM((8 * OUT_PITCH, 128), F32)],
        ),
        compiler_params=pltpu.CompilerParams(dimension_semantics=("arbitrary",), vmem_limit_bytes=56 * 2 ** 20),
        name="project",
    )(index, rows, norm_scale.reshape(1, -1), w_query, w_key, w_value, cosines, sines)


def solution(mesh):
    def local_step(token_ids, positions, table_rows, norm_scale, w_query, w_key, w_value):
        me = lax.axis_index("tp")
        vocab_rows, model_width = table_rows.shape
        scale = float(np.asarray(math.sqrt(model_width)).astype(BF16))
        tokens = token_ids.shape[0]
        index, own_list, count, fits = plan(token_ids, vocab_rows, me)
        fits_all = lax.pmin(fits.astype(I32), "dp")

        def compact_step(token_ids, positions, table_rows, norm_scale, w_query, w_key, w_value, index, own_list, count):
            base = jnp.asarray(SEG_BASE, I32)[me]
            hot_steps = jnp.where(me == 0, HOT // STEP, 0)
            params = jnp.stack([hot_steps, (count + STEP - 1) // STEP, base]).astype(I32)
            rows = gather_rows(params, own_list, table_rows, ROWS, None, "pick_rows")
            rows = broadcast_rows(rows)
            own_tokens = tokens // 8
            own_index = lax.dynamic_slice_in_dim(index, me * own_tokens, own_tokens)
            resid_params = jnp.asarray([0, own_tokens // STEP, 0], I32)
            residual = gather_rows(resid_params, own_index, rows, own_tokens, scale, "residual_rows")
            cosines, sines = rope_tables(positions)
            queries, keys, values = project(index, rows, norm_scale, w_query, w_key, w_value, cosines, sines, scale)
            return residual, queries, keys, values

        def dense(token_ids, positions, table_rows, norm_scale, w_query, w_key, w_value, *_):
            return dense_step(token_ids, positions, table_rows, norm_scale, w_query, w_key, w_value)

        residual, queries, keys, values = lax.cond(
            fits_all == 1, compact_step, dense,
            token_ids, positions, table_rows, norm_scale, w_query, w_key, w_value, index, own_list, count)
        return residual, queries[:, None, :], keys[:, None, :], values[:, None, :]

    head_spec = P("dp", "tp", None)
    return jax.shard_map(local_step, mesh=mesh, in_specs=(P("dp"), P("dp"), P("tp", None), P(), P(None, "tp"), P(), P()), out_specs=(P(("dp", "tp"), None), head_spec, head_spec, head_spec), check_vma=False)
```

```python
import functools
import math

import jax
import numpy as np
import jax.numpy as jnp
from jax import lax
from jax.experimental import pallas as pl
from jax.experimental.pallas import tpu as pltpu
from jax.sharding import PartitionSpec as P

HEAD_DIM = 256
EPSILON = 1e-6
ROPE_BASE = 10000.0
MESH = pl.DeviceIdType.MESH
BF16, F32, I32 = jnp.bfloat16, jnp.float32, jnp.int32

CHUNK = 64
HOT = 1024
LIST_CAP = (2816, 640, 384, 384, 192, 192, 192, 192)
SEG_ROWS = tuple(c + (HOT if d == 0 else 0) for d, c in enumerate(LIST_CAP))
SEG_BASE = tuple(sum(SEG_ROWS[:d]) for d in range(8))
ROWS = sum(SEG_ROWS)
SEG_CHUNKS = tuple(r // CHUNK for r in SEG_ROWS)
CHUNK_ID = tuple(b // CHUNK for b in SEG_BASE)
ALL_CHUNKS = ROWS // CHUNK
STEPS = ALL_CHUNKS // 2
SPLIT = STEPS - SEG_CHUNKS[2] - SEG_CHUNKS[4] - SEG_CHUNKS[6]
LIST_LEN = -(-max(LIST_CAP) // 128) * 128
RING = ((0, 1, 3, 2), (0, 2, 3, 1))


def rope_tables(positions):
    inv_freq = ROPE_BASE ** (-jnp.arange(0, HEAD_DIM, 2, dtype=F32) / HEAD_DIM)
    angles = positions.astype(F32)[:, None] * inv_freq[None, :]
    return jnp.cos(angles), jnp.sin(angles)


def rotate(head_vals, cosines, sines):
    half_dim = head_vals.shape[-1] // 2
    front_half = head_vals[..., :half_dim]
    back_half = head_vals[..., half_dim:]
    return jnp.concatenate([front_half * cosines - back_half * sines, back_half * cosines + front_half * sines], axis=-1)


def rms_norm(resid_rows, norm_scale):
    widened = resid_rows.astype(F32)
    inv_rms = lax.rsqrt(jnp.mean(widened * widened, axis=-1, keepdims=True) + EPSILON)
    return (widened * inv_rms * (1.0 + norm_scale)).astype(BF16)


def dense_step(token_ids, positions, table_rows, norm_scale, w_query, w_key, w_value):
    vocab_rows, model_width = table_rows.shape
    normalizer = jnp.asarray(math.sqrt(model_width), dtype=BF16)
    local_ids = token_ids - lax.axis_index("tp") * vocab_rows
    inside = (local_ids >= 0) & (local_ids < vocab_rows)
    picked = jnp.take(table_rows, local_ids, axis=0, mode="clip") * normalizer
    partial = jnp.where(inside[:, None], picked, jnp.zeros((), BF16))
    group = lax.axis_size("tp")
    blocks = lax.all_to_all(partial.reshape(group, -1, model_width), "tp", 0, 0)
    residual = jnp.sum(blocks.astype(F32), axis=0).astype(BF16)
    spread = jnp.broadcast_to(rms_norm(residual, norm_scale)[None], blocks.shape)
    normed = lax.all_to_all(spread, "tp", 0, 0).reshape(-1, model_width)
    cosines, sines = rope_tables(positions)

    def project(weight, factor):
        linear = jnp.dot(normed, weight, preferred_element_type=F32).astype(BF16).astype(F32)
        return (rotate(linear, cosines, sines) * factor).astype(BF16)

    value_heads = jnp.dot(normed, w_value, preferred_element_type=F32).astype(BF16)
    return residual, project(w_query, HEAD_DIM ** -0.5), project(w_key, 1.0), value_heads


def plan_kernel(vocab_rows, ids_ref, index_out, list_out, counts_out, own_place, own_high, own_low):
    me = lax.axis_index("tp")
    ids = ids_ref[...]
    rows, lanes = ids.shape
    owner = jnp.zeros_like(ids)
    for d in range(1, 8):
        owner += (ids >= d * vocab_rows).astype(I32)
    hot = ids < HOT
    owner = jnp.where(hot, 8, owner)
    marks = [(owner == d).astype(F32) for d in range(8)]
    stacked = jnp.concatenate(marks, axis=0).astype(BF16)
    row_of = lax.broadcasted_iota(I32, (lanes, lanes), 0)
    lane_of = lax.broadcasted_iota(I32, (lanes, lanes), 1)
    upper = (row_of < lane_of).astype(F32).astype(BF16)
    within = jnp.dot(stacked, upper, preferred_element_type=F32)
    per_row = jnp.dot(stacked, jnp.ones((lanes, lanes), BF16), preferred_element_type=F32)
    lower = (lax.broadcasted_iota(I32, (rows, rows), 0) > lax.broadcasted_iota(I32, (rows, rows), 1)).astype(F32).astype(BF16)
    index = jnp.where(hot, ids, 0).astype(F32)
    place = jnp.zeros((rows, lanes), F32)
    for d in range(8):
        here = slice(rows * d, rows * d + rows)
        before = jnp.dot(lower, per_row[here].astype(BF16), preferred_element_type=F32)
        at = within[here] + before
        place += marks[d] * at
        index += marks[d] * (at + float(SEG_BASE[d] + (HOT if d == 0 else 0)))
        counts_out[d:d + 1, :] = jnp.sum(per_row[here], axis=0, keepdims=True).astype(I32)
    index_out[...] = jnp.clip(index.astype(I32), 0, ROWS - 1)
    local = ids - me * vocab_rows
    own_place[...] = jnp.where(owner == me, place.astype(I32), -1)
    own_high[...] = lax.shift_right_logical(local, 8).astype(F32)
    own_low[...] = (local & 255).astype(F32)
    tall = list_out.shape[0]

    def scatter(r, total):
        at = own_place[pl.ds(r, 1), :]
        column = lax.broadcasted_iota(I32, (128, lanes), 0)
        high = (lax.broadcasted_iota(I32, (tall, lanes), 0) == lax.shift_right_arithmetic(at, 7)).astype(F32).astype(BF16)
        low = (column == (at & 127)).astype(F32)
        values = jnp.concatenate([low * own_high[pl.ds(r, 1), :], low * own_low[pl.ds(r, 1), :]], axis=0).astype(BF16)
        return total + lax.dot_general(high, values, (((1,), (1,)), ((), ())), preferred_element_type=F32)

    total = lax.fori_loop(0, rows, scatter, jnp.zeros((tall, 256), F32), unroll=4)
    list_out[...] = (total[:, :128] * 256.0 + total[:, 128:]).astype(I32)


def plan(token_ids, vocab_rows):
    tokens = token_ids.shape[0]
    square = (tokens // 128, 128)
    return pl.pallas_call(
        functools.partial(plan_kernel, vocab_rows),
        out_shape=(
            jax.ShapeDtypeStruct(square, I32),
            jax.ShapeDtypeStruct((LIST_LEN // 128, 128), I32),
            jax.ShapeDtypeStruct((8, 128), I32),
        ),
        scratch_shapes=[pltpu.VMEM(square, I32), pltpu.VMEM(square, F32), pltpu.VMEM(square, F32)],
        name="plan",
    )(token_ids.reshape(square))


STEP = 128
DEPTH = 4


def gather_kernel(scale, params, rows_list, lanes_list, source, out, groups, picked, in_sems, out_sems):
    first, end = params[0], params[1]

    def issue(step, slot):
        def one(t, _):
            group = lax.shift_right_logical(rows_list[(first + step) * STEP + t], 3)
            pltpu.make_async_copy(source.at[pl.ds(pl.multiple_of(group * 8, 8), 8)], groups.at[slot, pl.ds(pl.multiple_of(t * 8, 8), 8)], in_sems.at[slot]).start()
            return 0

        lax.fori_loop(0, STEP, one, 0, unroll=8)

    def arrive(slot):
        pltpu.make_async_copy(source.at[pl.ds(0, STEP * 8)], groups.at[slot], in_sems.at[slot]).wait()

    def drain(slot):
        pltpu.make_async_copy(picked.at[slot], out.at[pl.ds(0, STEP)], out_sems.at[slot]).wait()

    for ahead in range(DEPTH - 1):
        pl.when(ahead < end)(functools.partial(issue, ahead, ahead))

    def body(step, _):
        slot, put = lax.rem(step, DEPTH), lax.rem(step, 2)
        free = lax.rem(step + DEPTH - 1, DEPTH)
        arrive(slot)

        @pl.when(step + DEPTH - 1 < end)
        def _():
            issue(step + DEPTH - 1, free)

        @pl.when(step >= 2)
        def _():
            drain(put)

        within = lanes_list[pl.ds(first + step, 1), :] & 7
        target = lax.broadcasted_iota(I32, (1, STEP), 1) * 8 + within
        target = jnp.broadcast_to(target, (STEP, STEP)).T
        lane = lax.broadcasted_iota(I32, (STEP, STEP), 1)
        select = jnp.concatenate([(lane + STEP * j == target).astype(F32).astype(BF16) for j in range(8)], axis=1)
        for c in range(8):
            rows = jnp.dot(select, groups[slot, :, 256 * c:256 * c + 256], preferred_element_type=F32)
            picked[put, :, 256 * c:256 * c + 256] = (rows if scale is None else rows * scale).astype(BF16)
        pltpu.make_async_copy(picked.at[put], out.at[pl.ds(pl.multiple_of(step * STEP, STEP), STEP)], out_sems.at[put]).start()
        return 0

    lax.fori_loop(0, end, body, 0)
    @pl.when(end >= 2)
    def _():
        drain(lax.rem(end, 2))

    @pl.when(end >= 1)
    def _():
        drain(lax.rem(end + 1, 2))


def gather_rows(params, rows_list, source, out_rows, scale, name):
    return pl.pallas_call(
        functools.partial(gather_kernel, scale),
        out_shape=jax.ShapeDtypeStruct((out_rows, source.shape[1]), BF16),
        in_specs=[
            pl.BlockSpec(memory_space=pltpu.SMEM),
            pl.BlockSpec(memory_space=pltpu.SMEM),
            pl.BlockSpec(memory_space=pltpu.VMEM),
            pl.BlockSpec(memory_space=pl.ANY),
        ],
        out_specs=pl.BlockSpec(memory_space=pl.ANY),
        scratch_shapes=[
            pltpu.VMEM((DEPTH, STEP * 8, 2048), BF16),
            pltpu.VMEM((2, STEP, 2048), BF16),
            pltpu.SemaphoreType.DMA((DEPTH,)),
            pltpu.SemaphoreType.DMA((2,)),
        ],
        name=name,
    )(params, rows_list.reshape(-1), rows_list, source)


def ring_device(core, place):
    return 2 * RING[core][place % 4] + core


def ring_runs(core, place):
    if place % 4:
        device = ring_device(core, place)
        return [(CHUNK_ID[device], SEG_CHUNKS[device])]
    if core == 0:
        return [(0, SPLIT)]
    return [(CHUNK_ID[1], SEG_CHUNKS[1]), (SPLIT, SEG_CHUNKS[0] - SPLIT)]


def stream(device):
    core = device % 2
    place = RING[core].index(device // 2)
    return [first + i for back in range(4) for first, n in ring_runs(core, place - back) for i in range(n)]


def runs_of(numbers):
    runs = []
    for step, number in enumerate(numbers):
        if not runs or numbers[step - 1] + 1 != number:
            runs.append((step, number - step))
    return runs


def pick(me, values):
    out = jnp.asarray(values[0], I32)
    for d in range(1, len(values)):
        out = jnp.where(me == d, jnp.asarray(values[d], I32), out)
    return out


RING_RUNS = [runs_of(stream(d)) for d in range(8)]
PAIR_RUNS = [RING_RUNS[d ^ 1] for d in range(8)]
RUNS = max(len(r) for r in RING_RUNS)
TABLES = 64


def broadcast_kernel(scale, table, picked, norm_scale, w_query, w_key, w_value, positions, flags,
                     rows_out, linear_out, cos_out, sin_out, flags_out,
                     rows, linear, angles, ring_sems, pair_sems, recv_sems, load_sem, rows_sem, linear_sem, angle_sems, flag_sends, flag_recvs):
    me, plane = lax.axis_index("tp"), lax.axis_index("dp")
    core, chip = me % 2, me // 2
    x, y = chip % 2, chip // 2
    along_x = 2 * (2 * y + 1 - x) + core
    along_y = 2 * (2 * (1 - y) + x) + core
    pair = 2 * chip + 1 - core
    turn = (x + y + core) % 2
    after = turn * along_y + (1 - turn) * along_x
    barrier = pltpu.get_barrier_semaphore()
    for peer in (along_x, along_y, pair):
        pl.semaphore_signal(barrier, inc=1, device_id={"tp": peer}, device_id_type=MESH)
    for hop in (1, 2, 3):
        pl.semaphore_signal(barrier, inc=1, device_id={"dp": (plane + hop) % 4}, device_id_type=MESH)

    def chunk(number):
        return pl.ds(pl.multiple_of(number * CHUNK, CHUNK), CHUNK)

    own_first = pick(me, CHUNK_ID)
    own_list = own_first + jnp.where(me == 0, HOT // CHUNK, 0)
    own_end = own_first + pick(me, SEG_CHUNKS)

    def load_list(number, _):
        pltpu.make_async_copy(picked.at[chunk(number - own_list)], rows.at[chunk(number)], load_sem.at[number]).start()
        return 0

    @pl.when(me == 0)
    def _():
        def load_hot(number, _):
            pltpu.make_async_copy(table.at[chunk(number)], rows.at[chunk(number)], load_sem.at[number]).start()
            return 0

        lax.fori_loop(0, HOT // CHUNK, load_hot, 0)

    lax.fori_loop(own_list, own_end, load_list, 0)
    pl.semaphore_wait(barrier, 6)

    def flag_copy(hop):
        return pltpu.make_async_remote_copy(
            src_ref=flags, dst_ref=flags_out.at[hop], send_sem=flag_sends.at[hop], recv_sem=flag_recvs.at[hop],
            device_id={"dp": (plane + hop + 1) % 4}, device_id_type=MESH)

    for hop in range(3):
        flag_copy(hop).start()

    def copy(number, sems, target):
        return pltpu.make_async_remote_copy(
            src_ref=rows.at[chunk(number)], dst_ref=rows.at[chunk(number)], send_sem=sems.at[number], recv_sem=recv_sems.at[number],
            device_id={"tp": target}, device_id_type=MESH)

    def to_ring(number):
        copy(number, ring_sems, after).start()

    def to_pair(number):
        copy(number, pair_sems, pair).start()

    def keep(number):
        return pltpu.make_async_copy(rows.at[chunk(number)], rows_out.at[chunk(number)], rows_sem.at[number])

    def loaded(number):
        pltpu.make_async_copy(table.at[pl.ds(0, CHUNK)], rows.at[chunk(number)], load_sem.at[number]).wait()

    def send_own(number, _):
        loaded(number)
        to_pair(number)
        keep(number).start()

        @pl.when((me != 0) | (number < SPLIT))
        def _():
            to_ring(number)

        return 0

    @pl.when(me == 0)
    def _():
        ahead = SEG_CHUNKS[0] - SPLIT

        def both(i, _):
            send_own(SPLIT + i, 0)
            send_own(i, 0)
            return 0

        lax.fori_loop(0, ahead, both, 0)
        lax.fori_loop(ahead, SPLIT, send_own, 0)

    @pl.when(me != 0)
    def _():
        lax.fori_loop(own_first, own_end, send_own, 0)

    def number_at(step, all_runs):
        number = jnp.asarray(0, I32)
        for d in range(8):
            mine = jnp.asarray(all_runs[d][0][1], I32)
            for opens, shift in all_runs[d][1:]:
                mine = jnp.where(step >= opens, shift, mine)
            number = jnp.where(me == d, mine, number)
        return number + step

    last_first = pick(me, [len(stream(d)) - sum(n for _, n in ring_runs(d % 2, RING[d % 2].index(d // 2) - 3)) for d in range(8)])
    inv_freq = jnp.exp(lax.broadcasted_iota(I32, (1, 128), 1).astype(F32) * (-2.0 * math.log(ROPE_BASE) / HEAD_DIM))

    def project(number):
        resid = (rows[chunk(number), :].astype(F32) * scale).astype(BF16).astype(F32)
        inv_rms = lax.rsqrt(jnp.mean(resid * resid, axis=-1, keepdims=True) + EPSILON)
        return (resid * inv_rms * (1.0 + norm_scale[...])).astype(BF16)

    def angle_copies(slot, block):
        there = pl.ds(pl.multiple_of(block * 128, 128), 128)
        return (pltpu.make_async_copy(angles.at[slot, 0], cos_out.at[there], angle_sems.at[slot, 0]),
                pltpu.make_async_copy(angles.at[slot, 1], sin_out.at[there], angle_sems.at[slot, 1]))

    def linear_copy(number):
        there = pl.ds(pl.multiple_of(number * (CHUNK * 8), CHUNK * 8), CHUNK * 8)
        return pltpu.make_async_copy(linear.at[there], linear_out.at[there], linear_sem)

    def put_linear(step):
        linear_copy(number_at(step, RING_RUNS)).start()
        linear_copy(number_at(step, PAIR_RUNS)).start()

    def step_body(step, _):
        ring_number = number_at(step, RING_RUNS)
        pair_number = number_at(step, PAIR_RUNS)
        own_ring = (ring_number >= own_first) & (ring_number < own_end)
        second = (me == 1) & (ring_number < CHUNK_ID[1])

        @pl.when(jnp.logical_not(own_ring))
        def _():
            copy(ring_number, ring_sems, after).wait_recv()

            @pl.when(step < last_first)
            def _():
                to_ring(ring_number)

            @pl.when(jnp.logical_not(second))
            def _():
                to_pair(ring_number)

            keep(ring_number).start()

        @pl.when((pair_number < own_first) | (pair_number >= own_end))
        def _():
            copy(pair_number, ring_sems, after).wait_recv()
            keep(pair_number).start()

        for b in range(2):
            block = step * 2 + b

            @pl.when(block < positions.shape[0])
            def _():
                where = jnp.broadcast_to(positions[pl.ds(block, 1), :].astype(F32), (128, 128)).T
                angle = where * inv_freq

                @pl.when(step >= 1)
                def _():
                    for c in angle_copies(b, block - 2):
                        c.wait()

                angles[b, 0] = jnp.cos(angle)
                angles[b, 1] = jnp.sin(angle)

        normed = jnp.concatenate([project(ring_number), project(pair_number)], axis=0)
        for which, weight in enumerate((w_query, w_key, w_value)):
            product = jnp.dot(normed, weight[...], preferred_element_type=F32).astype(BF16).astype(F32)
            for half in range(2):
                part = product[:, 128 * half:128 * half + 128]
                for number, mine in ((ring_number, part[:CHUNK]), (pair_number, part[CHUNK:])):
                    linear[pl.ds(number * (CHUNK * 8) + 2 * which + half, CHUNK, stride=8), :] = mine
        for b in range(2):
            block = step * 2 + b

            @pl.when(block < positions.shape[0])
            def _():
                for c in angle_copies(b, block):
                    c.start()

        @pl.when(step >= 1)
        def _():
            put_linear(step - 1)

        return 0

    lax.fori_loop(0, STEPS, step_body, 0)
    for b in range(2):
        for c in angle_copies(b, positions.shape[0] - 2 + b):
            c.wait()
    put_linear(STEPS - 1)
    for hop in range(3):
        flag_copy(hop).wait()

    def sent_to_ring(step, _):
        copy(number_at(step, RING_RUNS), ring_sems, after).wait_send()
        return 0

    def sent_to_pair(step, _):
        number = number_at(step, RING_RUNS)

        @pl.when((me != 1) | (number >= CHUNK_ID[1]) | (number < SPLIT))
        def _():
            copy(number, pair_sems, pair).wait_send()

        return 0

    lax.fori_loop(0, last_first, sent_to_ring, 0)
    lax.fori_loop(0, STEPS, sent_to_pair, 0)

    @pl.when(me == 0)
    def _():
        def sent(number, _):
            copy(number, pair_sems, pair).wait_send()
            return 0

        lax.fori_loop(SPLIT, SEG_CHUNKS[0], sent, 0)

    def kept(number, _):
        keep(number).wait()
        return 0

    lax.fori_loop(0, ALL_CHUNKS, kept, 0)
    pltpu.make_async_copy(linear, linear_out, linear_sem).wait()


def broadcast_project(table, picked, norm_scale, w_query, w_key, w_value, positions, flags, scale):
    tokens = positions.size
    vmem, anywhere = pl.BlockSpec(memory_space=pltpu.VMEM), pl.BlockSpec(memory_space=pl.ANY)
    return pl.pallas_call(
        functools.partial(broadcast_kernel, scale),
        out_shape=(
            jax.ShapeDtypeStruct((ROWS, 2048), BF16),
            jax.ShapeDtypeStruct((ROWS * 8, 128), F32),
            jax.ShapeDtypeStruct((tokens, 128), F32),
            jax.ShapeDtypeStruct((tokens, 128), F32),
            jax.ShapeDtypeStruct((3, 8, 128), F32),
        ),
        in_specs=[anywhere, anywhere] + [vmem] * 6,
        out_specs=(anywhere, anywhere, anywhere, anywhere, vmem),
        scratch_shapes=[
            pltpu.VMEM((ROWS, 2048), BF16),
            pltpu.VMEM((ROWS * 8, 128), F32),
            pltpu.VMEM((2, 2, 128, 128), F32),
            pltpu.SemaphoreType.DMA((ALL_CHUNKS,)),
            pltpu.SemaphoreType.DMA((ALL_CHUNKS,)),
            pltpu.SemaphoreType.DMA((ALL_CHUNKS,)),
            pltpu.SemaphoreType.DMA((ALL_CHUNKS,)),
            pltpu.SemaphoreType.DMA((ALL_CHUNKS,)),
            pltpu.SemaphoreType.DMA,
            pltpu.SemaphoreType.DMA((2, 2)),
            pltpu.SemaphoreType.DMA((3,)),
            pltpu.SemaphoreType.DMA((3,)),
        ],
        compiler_params=pltpu.CompilerParams(collective_id=0, has_side_effects=True, vmem_limit_bytes=60 * 2 ** 20),
        name="broadcast_project",
    )(table, picked, norm_scale.reshape(1, -1), w_query, w_key, w_value, positions, flags)


TOKEN_BLOCK = 512
OUT_PITCH = TOKEN_BLOCK + 4


def order_kernel(index, linear_in, cosines, sines, q_out, k_out, v_out, linear, turned, sems):
    step = pl.program_id(0)

    @pl.when(step == 0)
    def _():
        eighth = ROWS
        copies = [pltpu.make_async_copy(linear_in.at[pl.ds(j * eighth, eighth)], linear.at[pl.ds(j * eighth, eighth)], sems.at[j]) for j in range(8)]
        for c in copies:
            c.start()
        for c in copies:
            c.wait()

    def some(i, _):
        for u in range(32):
            row = index[step * TOKEN_BLOCK + i * 32 + u]
            turned[pl.ds(i * 32 + u, 8, stride=OUT_PITCH), :] = linear[pl.ds(pl.multiple_of(row * 8, 8), 8), :]
        return 0

    lax.fori_loop(0, TOKEN_BLOCK // 32, some, 0)
    part = [turned[OUT_PITCH * j:OUT_PITCH * j + TOKEN_BLOCK, :] for j in range(6)]
    cos, sin = cosines[...], sines[...]
    factor = HEAD_DIM ** -0.5
    q_out[:, :128] = ((part[0] * cos - part[1] * sin) * factor).astype(BF16)
    q_out[:, 128:] = ((part[1] * cos + part[0] * sin) * factor).astype(BF16)
    k_out[:, :128] = (part[2] * cos - part[3] * sin).astype(BF16)
    k_out[:, 128:] = (part[3] * cos + part[2] * sin).astype(BF16)
    v_out[:, :128] = part[4].astype(BF16)
    v_out[:, 128:] = part[5].astype(BF16)


def token_order(index, linear, cosines, sines):
    tokens = cosines.shape[0]
    by_token = lambda i, idx: (i, 0)
    out = jax.ShapeDtypeStruct((tokens, HEAD_DIM), BF16)
    return pl.pallas_call(
        order_kernel,
        out_shape=(out, out, out),
        grid_spec=pltpu.PrefetchScalarGridSpec(
            num_scalar_prefetch=1,
            grid=(tokens // TOKEN_BLOCK,),
            in_specs=[
                pl.BlockSpec(memory_space=pl.ANY),
                pl.BlockSpec((TOKEN_BLOCK, 128), by_token),
                pl.BlockSpec((TOKEN_BLOCK, 128), by_token),
            ],
            out_specs=[pl.BlockSpec((TOKEN_BLOCK, HEAD_DIM), by_token)] * 3,
            scratch_shapes=[pltpu.VMEM((8 * ROWS, 128), F32), pltpu.VMEM((8 * OUT_PITCH, 128), F32), pltpu.SemaphoreType.DMA((8,))],
        ),
        compiler_params=pltpu.CompilerParams(dimension_semantics=("arbitrary",), vmem_limit_bytes=48 * 2 ** 20),
        name="token_order",
    )(index, linear, cosines, sines)


def solution(mesh):
    def local_step(token_ids, positions, table_rows, norm_scale, w_query, w_key, w_value):
        me = lax.axis_index("tp")
        vocab_rows, model_width = table_rows.shape
        scale = float(np.asarray(math.sqrt(model_width)).astype(BF16))
        tokens = token_ids.shape[0]
        index, own_list, counts = plan(token_ids, vocab_rows)
        length = counts[:, 0]
        fits = jnp.all(length <= jnp.asarray(LIST_CAP, I32))
        steps = jnp.minimum((length[me] + STEP - 1) // STEP, LIST_LEN // STEP)
        picked = gather_rows(jnp.stack([0, steps]).astype(I32), own_list, table_rows, LIST_LEN, None, "pick_rows")
        flags = jnp.broadcast_to(fits.astype(F32), (8, 128))
        rows, linear, cosines, sines, others = broadcast_project(
            table_rows, picked, norm_scale, w_query, w_key, w_value, positions.reshape(-1, 128), flags, scale)
        fits_all = fits & jnp.all(others[:, 0, 0] > 0.5)

        def compact_step(token_ids, positions, table_rows, norm_scale, w_query, w_key, w_value, index, rows, linear, cosines, sines):
            own_tokens = tokens // 8
            resid_params = jnp.stack([me * (own_tokens // STEP), own_tokens // STEP]).astype(I32)
            residual = gather_rows(resid_params, index, rows, own_tokens, scale, "residual_rows")
            queries, keys, values = token_order(index.reshape(tokens), linear, cosines, sines)
            return residual, queries, keys, values

        def dense(token_ids, positions, table_rows, norm_scale, w_query, w_key, w_value, *_):
            return dense_step(token_ids, positions, table_rows, norm_scale, w_query, w_key, w_value)

        residual, queries, keys, values = lax.cond(
            fits_all, compact_step, dense,
            token_ids, positions, table_rows, norm_scale, w_query, w_key, w_value, index, rows, linear, cosines, sines)
        return residual, queries[:, None, :], keys[:, None, :], values[:, None, :]

    head_spec = P("dp", "tp", None)
    return jax.shard_map(local_step, mesh=mesh, in_specs=(P("dp"), P("dp"), P("tp", None), P(), P(None, "tp"), P(), P()), out_specs=(P(("dp", "tp"), None), head_spec, head_spec, head_spec), check_vma=False)
```

```python
import functools
import math

import jax
import numpy as np
import jax.numpy as jnp
from jax import lax
from jax.experimental import pallas as pl
from jax.experimental.pallas import tpu as pltpu
from jax.sharding import PartitionSpec as P

HEAD_DIM = 256
EPSILON = 1e-6
ROPE_BASE = 10000.0
MESH = pl.DeviceIdType.MESH
BF16, F32, I32 = jnp.bfloat16, jnp.float32, jnp.int32

CHUNK = 64
HOT = 1024
LIST_CAP = (2816, 640, 320, 320, 192, 192, 192, 192)
SEG_ROWS = tuple(c + (HOT if d == 0 else 0) for d, c in enumerate(LIST_CAP))
SEG_BASE = tuple(sum(SEG_ROWS[:d]) for d in range(8))
ROWS = sum(SEG_ROWS)
SEG_CHUNKS = tuple(r // CHUNK for r in SEG_ROWS)
CHUNK_ID = tuple(b // CHUNK for b in SEG_BASE)
ALL_CHUNKS = ROWS // CHUNK
STEPS = ALL_CHUNKS // 2
SPLIT = STEPS - SEG_CHUNKS[2] - SEG_CHUNKS[4] - SEG_CHUNKS[6]
LIST_LEN = -(-max(LIST_CAP) // 128) * 128
RING = ((0, 1, 3, 2), (0, 2, 3, 1))


def rope_tables(positions):
    inv_freq = ROPE_BASE ** (-jnp.arange(0, HEAD_DIM, 2, dtype=F32) / HEAD_DIM)
    angles = positions.astype(F32)[:, None] * inv_freq[None, :]
    return jnp.cos(angles), jnp.sin(angles)


def rotate(head_vals, cosines, sines):
    half_dim = head_vals.shape[-1] // 2
    front_half = head_vals[..., :half_dim]
    back_half = head_vals[..., half_dim:]
    return jnp.concatenate([front_half * cosines - back_half * sines, back_half * cosines + front_half * sines], axis=-1)


def rms_norm(resid_rows, norm_scale):
    widened = resid_rows.astype(F32)
    inv_rms = lax.rsqrt(jnp.mean(widened * widened, axis=-1, keepdims=True) + EPSILON)
    return (widened * inv_rms * (1.0 + norm_scale)).astype(BF16)


def dense_step(token_ids, positions, table_rows, norm_scale, w_query, w_key, w_value):
    vocab_rows, model_width = table_rows.shape
    normalizer = jnp.asarray(math.sqrt(model_width), dtype=BF16)
    local_ids = token_ids - lax.axis_index("tp") * vocab_rows
    inside = (local_ids >= 0) & (local_ids < vocab_rows)
    picked = jnp.take(table_rows, local_ids, axis=0, mode="clip") * normalizer
    partial = jnp.where(inside[:, None], picked, jnp.zeros((), BF16))
    group = lax.axis_size("tp")
    blocks = lax.all_to_all(partial.reshape(group, -1, model_width), "tp", 0, 0)
    residual = jnp.sum(blocks.astype(F32), axis=0).astype(BF16)
    spread = jnp.broadcast_to(rms_norm(residual, norm_scale)[None], blocks.shape)
    normed = lax.all_to_all(spread, "tp", 0, 0).reshape(-1, model_width)
    cosines, sines = rope_tables(positions)

    def project(weight, factor):
        linear = jnp.dot(normed, weight, preferred_element_type=F32).astype(BF16).astype(F32)
        return (rotate(linear, cosines, sines) * factor).astype(BF16)

    value_heads = jnp.dot(normed, w_value, preferred_element_type=F32).astype(BF16)
    return residual, project(w_query, HEAD_DIM ** -0.5), project(w_key, 1.0), value_heads


def plan_kernel(vocab_rows, ids_ref, index_out, list_out, flags_out, steps_out, own_place, own_high, own_low):
    me = lax.axis_index("tp")
    ids = ids_ref[...]
    rows, lanes = ids.shape
    owner = jnp.zeros_like(ids)
    for d in range(1, 8):
        owner += (ids >= d * vocab_rows).astype(I32)
    hot = ids < HOT
    owner = jnp.where(hot, 8, owner)
    marks = [(owner == d).astype(F32) for d in range(8)]
    stacked = jnp.concatenate(marks, axis=0).astype(BF16)
    row_of = lax.broadcasted_iota(I32, (lanes, lanes), 0)
    lane_of = lax.broadcasted_iota(I32, (lanes, lanes), 1)
    upper = (row_of < lane_of).astype(F32).astype(BF16)
    within = jnp.dot(stacked, upper, preferred_element_type=F32)
    per_row = jnp.dot(stacked, jnp.ones((lanes, lanes), BF16), preferred_element_type=F32)
    lower = (lax.broadcasted_iota(I32, (rows, rows), 0) > lax.broadcasted_iota(I32, (rows, rows), 1)).astype(F32).astype(BF16)
    index = jnp.where(hot, ids, 0).astype(F32)
    place = jnp.zeros((rows, lanes), F32)
    fits = jnp.ones((1, lanes), F32)
    for d in range(8):
        here = slice(rows * d, rows * d + rows)
        before = jnp.dot(lower, per_row[here].astype(BF16), preferred_element_type=F32)
        at = within[here] + before
        place += marks[d] * at
        index += marks[d] * (at + float(SEG_BASE[d] + (HOT if d == 0 else 0)))
        fits *= (jnp.sum(per_row[here], axis=0, keepdims=True) <= float(LIST_CAP[d])).astype(F32)
    index_out[...] = jnp.clip(index.astype(I32), 0, ROWS - 1)
    flags_out[...] = jnp.broadcast_to(fits, flags_out.shape)
    length = jnp.sum((owner == me).astype(F32)).astype(I32)
    steps_out[0] = jnp.minimum(lax.shift_right_logical(length + 127, 7), LIST_LEN // 128)
    local = ids - me * vocab_rows
    own_place[...] = jnp.where(owner == me, place.astype(I32), -1)
    own_high[...] = lax.shift_right_logical(local, 8).astype(F32)
    own_low[...] = (local & 255).astype(F32)
    tall = list_out.shape[0]

    def scatter(r, total):
        at = own_place[pl.ds(r, 1), :]
        column = lax.broadcasted_iota(I32, (128, lanes), 0)
        high = (lax.broadcasted_iota(I32, (tall, lanes), 0) == lax.shift_right_arithmetic(at, 7)).astype(F32).astype(BF16)
        low = (column == (at & 127)).astype(F32)
        values = jnp.concatenate([low * own_high[pl.ds(r, 1), :], low * own_low[pl.ds(r, 1), :]], axis=0).astype(BF16)
        return total + lax.dot_general(high, values, (((1,), (1,)), ((), ())), preferred_element_type=F32)

    total = lax.fori_loop(0, rows, scatter, jnp.zeros((tall, 256), F32), unroll=4)
    list_out[...] = (total[:, :128] * 256.0 + total[:, 128:]).astype(I32)


def plan(token_ids, vocab_rows):
    tokens = token_ids.shape[0]
    square = (tokens // 128, 128)
    return pl.pallas_call(
        functools.partial(plan_kernel, vocab_rows),
        out_shape=(
            jax.ShapeDtypeStruct(square, I32),
            jax.ShapeDtypeStruct((LIST_LEN // 128, 128), I32),
            jax.ShapeDtypeStruct((8, 128), F32),
            jax.ShapeDtypeStruct((1,), I32),
        ),
        out_specs=tuple(pl.BlockSpec(memory_space=space) for space in (pltpu.VMEM, pltpu.VMEM, pltpu.VMEM, pltpu.SMEM)),
        scratch_shapes=[pltpu.VMEM(square, I32), pltpu.VMEM(square, F32), pltpu.VMEM(square, F32)],
        name="plan",
    )(token_ids.reshape(square))


STEP = 128
DEPTH = 4


def gather(scale, first, end, rows_list, lanes_list, source, out, groups, picked, in_sems, out_sems):
    def one(at, slot, t):
        group = lax.shift_right_logical(rows_list[at + t], 3)
        pltpu.make_async_copy(source.at[pl.ds(pl.multiple_of(group * 8, 8), 8)], groups.at[slot, pl.ds(pl.multiple_of(t * 8, 8), 8)], in_sems.at[slot]).start()

    def issue(step, slot):
        def some(i, _):
            for u in range(16):
                one((first + step) * STEP, slot, i * 16 + u)
            return 0

        lax.fori_loop(0, STEP // 16, some, 0)

    def drain(slot):
        pltpu.make_async_copy(picked.at[slot], out.at[pl.ds(0, STEP)], out_sems.at[slot]).wait()

    def opening():
        for ahead in range(DEPTH - 1):
            pl.when(ahead < end)(functools.partial(issue, ahead, ahead))

    def body(step, _):
        slot, put = lax.rem(step, DEPTH), lax.rem(step, 2)
        free = lax.rem(step + DEPTH - 1, DEPTH)
        pltpu.make_async_copy(source.at[pl.ds(0, STEP * 8)], groups.at[slot], in_sems.at[slot]).wait()

        @pl.when(step + DEPTH - 1 < end)
        def _():
            issue(step + DEPTH - 1, free)

        @pl.when(step >= 2)
        def _():
            drain(put)

        within = lanes_list[pl.ds(first + step, 1), :] & 7
        target = lax.broadcasted_iota(I32, (1, STEP), 1) * 8 + within
        target = jnp.broadcast_to(target, (STEP, STEP)).T
        lane = lax.broadcasted_iota(I32, (STEP, STEP), 1)
        select = jnp.concatenate([(lane + STEP * j == target).astype(F32).astype(BF16) for j in range(8)], axis=1)
        for c in range(0, 2048, 256):
            rows = jnp.dot(select, groups[slot, :, c:c + 256], preferred_element_type=F32)
            picked[put, :, c:c + 256] = (rows if scale is None else rows * scale).astype(BF16)
        pltpu.make_async_copy(picked.at[put], out.at[pl.ds(pl.multiple_of(step * STEP, STEP), STEP)], out_sems.at[put]).start()
        return 0

    def close():
        @pl.when(end >= 2)
        def _():
            drain(lax.rem(end, 2))

        @pl.when(end >= 1)
        def _():
            drain(lax.rem(end + 1, 2))

    return opening, body, close


GATHER_SCRATCH = [
    pltpu.VMEM((DEPTH, STEP * 8, 2048), BF16),
    pltpu.VMEM((2, STEP, 2048), BF16),
    pltpu.SemaphoreType.DMA((DEPTH,)),
    pltpu.SemaphoreType.DMA((2,)),
]


def pick_kernel(steps, rows_list, lanes_list, source, out, *scratch):
    end = steps[0]
    opening, body, close = gather(None, 0, end, rows_list, lanes_list, source, out, *scratch)
    opening()
    lax.fori_loop(0, end, body, 0)
    close()


def pick_rows(steps, rows_list, source):
    smem, vmem, anywhere = (pl.BlockSpec(memory_space=space) for space in (pltpu.SMEM, pltpu.VMEM, pl.ANY))
    return pl.pallas_call(
        pick_kernel,
        out_shape=jax.ShapeDtypeStruct((LIST_LEN, source.shape[1]), BF16),
        in_specs=[smem, smem, vmem, anywhere],
        out_specs=anywhere,
        scratch_shapes=GATHER_SCRATCH,
        name="pick_rows",
    )(steps, rows_list.reshape(-1), rows_list, source)


def ring_device(core, place):
    return 2 * RING[core][place % 4] + core


def ring_runs(core, place):
    if place % 4:
        device = ring_device(core, place)
        return [(CHUNK_ID[device], SEG_CHUNKS[device])]
    if core == 0:
        return [(0, SPLIT)]
    return [(CHUNK_ID[1], SEG_CHUNKS[1]), (SPLIT, SEG_CHUNKS[0] - SPLIT)]


def stream(device):
    core = device % 2
    place = RING[core].index(device // 2)
    return [first + i for back in range(4) for first, n in ring_runs(core, place - back) for i in range(n)]


def runs_of(numbers):
    runs = []
    for step, number in enumerate(numbers):
        if not runs or numbers[step - 1] + 1 != number:
            runs.append((step, number - step))
    return runs


def pick(me, values):
    out = jnp.asarray(values[0], I32)
    for d in range(1, len(values)):
        out = jnp.where(me == d, jnp.asarray(values[d], I32), out)
    return out


RING_RUNS = [runs_of(stream(d)) for d in range(8)]
PAIR_RUNS = [RING_RUNS[d ^ 1] for d in range(8)]
RUNS = max(len(r) for r in RING_RUNS)
TABLES = 64


def broadcast_kernel(scale, table, picked, norm_scale, w_query, w_key, w_value, positions, flags,
                     rows_out, linear_out, cos_out, sin_out, flags_out,
                     rows, linear, angles, flags_in, ring_sems, pair_sems, recv_sems, load_sem, rows_sem, linear_sem, angle_sems, flag_sends, flag_recvs):
    me, plane = lax.axis_index("tp"), lax.axis_index("dp")
    core, chip = me % 2, me // 2
    x, y = chip % 2, chip // 2
    along_x = 2 * (2 * y + 1 - x) + core
    along_y = 2 * (2 * (1 - y) + x) + core
    pair = 2 * chip + 1 - core
    turn = (x + y + core) % 2
    after = turn * along_y + (1 - turn) * along_x
    barrier = pltpu.get_barrier_semaphore()
    for peer in (along_x, along_y, pair):
        pl.semaphore_signal(barrier, inc=1, device_id={"tp": peer}, device_id_type=MESH)
    for hop in (1, 2, 3):
        pl.semaphore_signal(barrier, inc=1, device_id={"dp": (plane + hop) % 4}, device_id_type=MESH)

    def chunk(number):
        return pl.ds(pl.multiple_of(number * CHUNK, CHUNK), CHUNK)

    own_first = pick(me, CHUNK_ID)
    own_list = own_first + jnp.where(me == 0, HOT // CHUNK, 0)
    own_end = own_first + pick(me, SEG_CHUNKS)

    def load_list(number, _):
        pltpu.make_async_copy(picked.at[chunk(number - own_list)], rows.at[chunk(number)], load_sem.at[number]).start()
        return 0

    @pl.when(me == 0)
    def _():
        def load_hot(number, _):
            load_list(SPLIT + number, 0)
            pltpu.make_async_copy(table.at[chunk(number)], rows.at[chunk(number)], load_sem.at[number]).start()
            return 0

        def load_both(number, _):
            load_list(SPLIT + number, 0)
            return load_list(number, 0)

        lax.fori_loop(0, HOT // CHUNK, load_hot, 0)
        lax.fori_loop(HOT // CHUNK, SEG_CHUNKS[0] - SPLIT, load_both, 0)
        lax.fori_loop(SEG_CHUNKS[0] - SPLIT, SPLIT, load_list, 0)

    @pl.when(me != 0)
    def _():
        lax.fori_loop(own_list, own_end, load_list, 0)

    pl.semaphore_wait(barrier, 6)

    def flag_copy(hop):
        return pltpu.make_async_remote_copy(
            src_ref=flags, dst_ref=flags_in.at[hop], send_sem=flag_sends.at[hop], recv_sem=flag_recvs.at[hop],
            device_id={"dp": (plane + hop + 1) % 4}, device_id_type=MESH)

    for hop in range(3):
        flag_copy(hop).start()

    def copy(number, sems, target):
        return pltpu.make_async_remote_copy(
            src_ref=rows.at[chunk(number)], dst_ref=rows.at[chunk(number)], send_sem=sems.at[number], recv_sem=recv_sems.at[number],
            device_id={"tp": target}, device_id_type=MESH)

    def to_ring(number):
        copy(number, ring_sems, after).start()

    def to_pair(number):
        copy(number, pair_sems, pair).start()

    def keep(number):
        return pltpu.make_async_copy(rows.at[chunk(number)], rows_out.at[chunk(number)], rows_sem.at[number])

    def loaded(number):
        pltpu.make_async_copy(table.at[pl.ds(0, CHUNK)], rows.at[chunk(number)], load_sem.at[number]).wait()

    def send_own(number, _):
        loaded(number)
        to_pair(number)
        keep(number).start()

        @pl.when((me != 0) | (number < SPLIT))
        def _():
            to_ring(number)

        return 0

    @pl.when(me == 0)
    def _():
        ahead = SEG_CHUNKS[0] - SPLIT

        def both(i, _):
            send_own(SPLIT + i, 0)
            send_own(i, 0)
            return 0

        lax.fori_loop(0, ahead, both, 0)
        lax.fori_loop(ahead, SPLIT, send_own, 0)

    @pl.when(me != 0)
    def _():
        lax.fori_loop(own_first, own_end, send_own, 0)

    def number_at(step, all_runs):
        number = jnp.asarray(0, I32)
        for d in range(8):
            mine = jnp.asarray(all_runs[d][0][1], I32)
            for opens, shift in all_runs[d][1:]:
                mine = jnp.where(step >= opens, shift, mine)
            number = jnp.where(me == d, mine, number)
        return number + step

    last_first = pick(me, [len(stream(d)) - sum(n for _, n in ring_runs(d % 2, RING[d % 2].index(d // 2) - 3)) for d in range(8)])
    inv_freq = jnp.exp(lax.broadcasted_iota(I32, (1, 128), 1).astype(F32) * (-2.0 * math.log(ROPE_BASE) / HEAD_DIM))

    def project(number):
        resid = (rows[chunk(number), :].astype(F32) * scale).astype(BF16).astype(F32)
        inv_rms = lax.rsqrt(jnp.mean(resid * resid, axis=-1, keepdims=True) + EPSILON)
        return (resid * inv_rms * (1.0 + norm_scale[...])).astype(BF16)

    def angle_copies(slot, block):
        there = pl.ds(pl.multiple_of(block * 128, 128), 128)
        return (pltpu.make_async_copy(angles.at[slot, 0], cos_out.at[there], angle_sems.at[slot, 0]),
                pltpu.make_async_copy(angles.at[slot, 1], sin_out.at[there], angle_sems.at[slot, 1]))

    def linear_copy(number):
        there = pl.ds(pl.multiple_of(number * (CHUNK * 8), CHUNK * 8), CHUNK * 8)
        return pltpu.make_async_copy(linear.at[there], linear_out.at[there], linear_sem)

    def put_linear(step):
        linear_copy(number_at(step, RING_RUNS)).start()
        linear_copy(number_at(step, PAIR_RUNS)).start()

    def step_body(step, _):
        ring_number = number_at(step, RING_RUNS)
        pair_number = number_at(step, PAIR_RUNS)
        own_ring = (ring_number >= own_first) & (ring_number < own_end)
        second = (me == 1) & (ring_number < CHUNK_ID[1])

        @pl.when(jnp.logical_not(own_ring))
        def _():
            copy(ring_number, ring_sems, after).wait_recv()

            @pl.when(step < last_first)
            def _():
                to_ring(ring_number)

            @pl.when(jnp.logical_not(second))
            def _():
                to_pair(ring_number)

            keep(ring_number).start()

        @pl.when((pair_number < own_first) | (pair_number >= own_end))
        def _():
            copy(pair_number, ring_sems, after).wait_recv()
            keep(pair_number).start()

        for b in range(2):
            block = step * 2 + b

            @pl.when(block < positions.shape[0])
            def _():
                where = jnp.broadcast_to(positions[pl.ds(block, 1), :].astype(F32), (128, 128)).T
                angle = where * inv_freq

                @pl.when(step >= 1)
                def _():
                    for c in angle_copies(b, block - 2):
                        c.wait()

                angles[b, 0] = jnp.cos(angle)
                angles[b, 1] = jnp.sin(angle)

        normed = jnp.concatenate([project(ring_number), project(pair_number)], axis=0)
        for which, weight in enumerate((w_query, w_key, w_value)):
            product = jnp.dot(normed, weight[...], preferred_element_type=F32).astype(BF16).astype(F32)
            for half in range(2):
                part = product[:, 128 * half:128 * half + 128]
                for number, mine in ((ring_number, part[:CHUNK]), (pair_number, part[CHUNK:])):
                    linear[pl.ds(number * (CHUNK * 8) + 2 * which + half, CHUNK, stride=8), :] = mine
        for b in range(2):
            block = step * 2 + b

            @pl.when(block < positions.shape[0])
            def _():
                for c in angle_copies(b, block):
                    c.start()

        @pl.when(step >= 1)
        def _():
            put_linear(step - 1)

        return 0

    lax.fori_loop(0, STEPS, step_body, 0)
    for b in range(2):
        for c in angle_copies(b, positions.shape[0] - 2 + b):
            c.wait()
    put_linear(STEPS - 1)
    for hop in range(3):
        flag_copy(hop).wait()
    flags_out[...] = jnp.minimum(jnp.minimum(flags[...], flags_in[0]), jnp.minimum(flags_in[1], flags_in[2]))

    def sent_to_ring(step, _):
        copy(number_at(step, RING_RUNS), ring_sems, after).wait_send()
        return 0

    def sent_to_pair(step, _):
        number = number_at(step, RING_RUNS)

        @pl.when((me != 1) | (number >= CHUNK_ID[1]) | (number < SPLIT))
        def _():
            copy(number, pair_sems, pair).wait_send()

        return 0

    lax.fori_loop(0, last_first, sent_to_ring, 0)
    lax.fori_loop(0, STEPS, sent_to_pair, 0)

    @pl.when(me == 0)
    def _():
        def sent(number, _):
            copy(number, pair_sems, pair).wait_send()
            return 0

        lax.fori_loop(SPLIT, SEG_CHUNKS[0], sent, 0)

    def kept(number, _):
        keep(number).wait()
        return 0

    lax.fori_loop(0, ALL_CHUNKS, kept, 0)
    pltpu.make_async_copy(linear, linear_out, linear_sem).wait()


def broadcast_project(table, picked, norm_scale, w_query, w_key, w_value, positions, flags, scale):
    tokens = positions.size
    vmem, anywhere = pl.BlockSpec(memory_space=pltpu.VMEM), pl.BlockSpec(memory_space=pl.ANY)
    return pl.pallas_call(
        functools.partial(broadcast_kernel, scale),
        out_shape=(
            jax.ShapeDtypeStruct((ROWS, 2048), BF16),
            jax.ShapeDtypeStruct((ROWS * 8, 128), F32),
            jax.ShapeDtypeStruct((tokens, 128), F32),
            jax.ShapeDtypeStruct((tokens, 128), F32),
            jax.ShapeDtypeStruct((8, 128), F32),
        ),
        in_specs=[anywhere, anywhere] + [vmem] * 6,
        out_specs=(anywhere, anywhere, anywhere, anywhere, vmem),
        scratch_shapes=[
            pltpu.VMEM((ROWS, 2048), BF16),
            pltpu.VMEM((ROWS * 8, 128), F32),
            pltpu.VMEM((2, 2, 128, 128), F32),
            pltpu.VMEM((3, 8, 128), F32),
            pltpu.SemaphoreType.DMA((ALL_CHUNKS,)),
            pltpu.SemaphoreType.DMA((ALL_CHUNKS,)),
            pltpu.SemaphoreType.DMA((ALL_CHUNKS,)),
            pltpu.SemaphoreType.DMA((ALL_CHUNKS,)),
            pltpu.SemaphoreType.DMA((ALL_CHUNKS,)),
            pltpu.SemaphoreType.DMA,
            pltpu.SemaphoreType.DMA((2, 2)),
            pltpu.SemaphoreType.DMA((3,)),
            pltpu.SemaphoreType.DMA((3,)),
        ],
        compiler_params=pltpu.CompilerParams(collective_id=0, has_side_effects=True, vmem_limit_bytes=60 * 2 ** 20),
        name="broadcast_project",
    )(table, picked, norm_scale.reshape(1, -1), w_query, w_key, w_value, positions, flags)


TOKEN_BLOCK = 1024
OUT_PITCH = TOKEN_BLOCK + 4


def order_kernel(scale, index, index_lanes, rows, linear_in, cosines, sines, resid_out, q_out, k_out, v_out, linear, turned, sems, *scratch):
    step = pl.program_id(0)
    own_steps = jnp.asarray(resid_out.shape[0] // STEP, I32)
    opening, body, close = gather(scale, lax.axis_index("tp") * own_steps, own_steps, index, index_lanes, rows, resid_out, *scratch)

    copies = [pltpu.make_async_copy(linear_in.at[pl.ds(j * ROWS, ROWS)], linear.at[pl.ds(j * ROWS, ROWS)], sems.at[j]) for j in range(8)]

    @pl.when(step == 0)
    def _():
        opening()
        for c in copies:
            c.start()

    @pl.when(step < own_steps)
    def _():
        body(step, 0)

    @pl.when(step == 0)
    def _():
        for c in copies:
            c.wait()

    def some(i, _):
        for u in range(32):
            row = index[step * TOKEN_BLOCK + i * 32 + u]
            turned[pl.ds(i * 32 + u, 8, stride=OUT_PITCH), :] = linear[pl.ds(pl.multiple_of(row * 8, 8), 8), :]
        return 0

    lax.fori_loop(0, TOKEN_BLOCK // 32, some, 0)
    part = [turned[OUT_PITCH * j:OUT_PITCH * j + TOKEN_BLOCK, :] for j in range(6)]
    cos, sin = cosines[...], sines[...]
    factor = HEAD_DIM ** -0.5
    q_out[:, :128] = ((part[0] * cos - part[1] * sin) * factor).astype(BF16)
    q_out[:, 128:] = ((part[1] * cos + part[0] * sin) * factor).astype(BF16)
    k_out[:, :128] = (part[2] * cos - part[3] * sin).astype(BF16)
    k_out[:, 128:] = (part[3] * cos + part[2] * sin).astype(BF16)
    v_out[:, :128] = part[4].astype(BF16)
    v_out[:, 128:] = part[5].astype(BF16)
    pl.when(step == pl.num_programs(0) - 1)(close)


def token_order(index, rows, linear, cosines, sines, scale):
    tokens = cosines.shape[0]
    by_token = lambda i, idx: (i, 0)
    out = jax.ShapeDtypeStruct((tokens, HEAD_DIM), BF16)
    vmem, anywhere = (pl.BlockSpec(memory_space=space) for space in (pltpu.VMEM, pl.ANY))
    return pl.pallas_call(
        functools.partial(order_kernel, scale),
        out_shape=(jax.ShapeDtypeStruct((tokens // 8, rows.shape[1]), BF16), out, out, out),
        grid_spec=pltpu.PrefetchScalarGridSpec(
            num_scalar_prefetch=1,
            grid=(tokens // TOKEN_BLOCK,),
            in_specs=[
                vmem, anywhere, anywhere,
                pl.BlockSpec((TOKEN_BLOCK, 128), by_token),
                pl.BlockSpec((TOKEN_BLOCK, 128), by_token),
            ],
            out_specs=[anywhere] + [pl.BlockSpec((TOKEN_BLOCK, HEAD_DIM), by_token)] * 3,
            scratch_shapes=[pltpu.VMEM((8 * ROWS, 128), F32), pltpu.VMEM((8 * OUT_PITCH, 128), F32), pltpu.SemaphoreType.DMA((8,))] + GATHER_SCRATCH,
        ),
        compiler_params=pltpu.CompilerParams(dimension_semantics=("arbitrary",), vmem_limit_bytes=60 * 2 ** 20),
        name="token_order",
    )(index.reshape(tokens), index, rows, linear, cosines, sines)


def solution(mesh):
    def local_step(token_ids, positions, table_rows, norm_scale, w_query, w_key, w_value):
        vocab_rows, model_width = table_rows.shape
        scale = float(np.asarray(math.sqrt(model_width)).astype(BF16))
        index, own_list, flags, steps = plan(token_ids, vocab_rows)
        picked = pick_rows(steps, own_list, table_rows)
        rows, linear, cosines, sines, flags = broadcast_project(
            table_rows, picked, norm_scale, w_query, w_key, w_value, positions.reshape(-1, 128), flags, scale)

        def compact_step(token_ids, positions, table_rows, norm_scale, w_query, w_key, w_value, index, rows, linear, cosines, sines):
            return token_order(index, rows, linear, cosines, sines, scale)

        def dense(token_ids, positions, table_rows, norm_scale, w_query, w_key, w_value, *_):
            return dense_step(token_ids, positions, table_rows, norm_scale, w_query, w_key, w_value)

        residual, queries, keys, values = lax.cond(
            flags[0, 0] > 0.5, compact_step, dense,
            token_ids, positions, table_rows, norm_scale, w_query, w_key, w_value, index, rows, linear, cosines, sines)
        return residual, queries[:, None, :], keys[:, None, :], values[:, None, :]

    head_spec = P("dp", "tp", None)
    return jax.shard_map(local_step, mesh=mesh, in_specs=(P("dp"), P("dp"), P("tp", None), P(), P(None, "tp"), P(), P()), out_specs=(P(("dp", "tp"), None), head_spec, head_spec, head_spec), check_vma=False)
```
